128 devices in a mesh: row: 16 (over z, x), col: 8 (over y, core).
Axes of the slice: x: 4, y: 4, z: 4, core: 2. Of those that a mesh axis runs over, the one named last changes fastest.
Arguments:
- pole_values: float32 [65536], P('row'), may hold values from -32768 to 32768, as said below
- weights: float32 [65536], P('row'), may hold values from 0.15 to 0.5
- centers: float32 [65536], P('col'), as said below
- offsets: float32 [65536], P('col'), may hold values from -0.1 to 0.1
- chosen: int32 [2048], replicated, may hold values from 0 to 65535
- column_pole: int32 [2, 32768], P(None, 'row'), may hold values from 0 to 65535, as said below
- eigen_blocks: bfloat16 [6144, 2, 32768], P('col', None, 'row'), may hold values from -6 to 6
Outputs:
- roots_offset: float32 [65536], P('col')
- panel: float32 [6144, 2, 2048], P(('col', 'row'))
The draws below stay inside these ranges and needn't reach their ends.
Inputs may be any that keep to these rules, and one draw needn't show every extreme that they name: `pole_values`: ascending; consecutive poles differ by 1/4 to 7/4; every pole is a multiple of 1/128. centers[i] is the midpoint of pole_values[i] and pole_values[i + 1]; the last one is the last pole plus 1/2. `chosen`: indices of roots. `column_pole`: each of 0 to 65535 stands once.
All inputs are finite; a program needn't handle non-finite values.
Results may differ from the reference program's by a relative error of at most 0.0021.
Values may be sent and summed in bfloat16 or wider, within the bound.
A program may use at most 128 MiB of HBM per device.

```python
import math
import jax
import jax.numpy as jnp
from jax import lax

N = 65536
H = 32768
ITERS = 3
K = 2048
QROWS = 6144


def pole_layout(key):
    marks = jax.random.randint(jax.random.fold_in(key, 11), (N,), 16, 113)
    return (jnp.arange(N) - N // 2).astype(jnp.float32) + marks.astype(jnp.float32) / 128.0


def draw_pole_values(key, part):
    return pole_layout(key)


def draw_centers(key, part):
    values = pole_layout(key)
    return jnp.concatenate([0.5 * (values[:-1] + values[1:]), values[-1:] + 0.5])


def draw_column_pole(key, part):
    return jax.random.permutation(jax.random.fold_in(key, 5), N).astype(jnp.int32).reshape(2, H)


def plant(drawn, stream_key, smallest, high):
    shape = drawn.shape
    place = [jax.random.randint(jax.random.fold_in(stream_key, axis), (), 0, shape[axis]) for axis in range(len(shape))]
    drawn = drawn.at[tuple(place)].set(smallest)
    longest = shape.index(max(shape))
    place[longest] = (place[longest] + 1) % shape[longest]
    return drawn.at[tuple(place)].set(high)


def steps_of(own_key, shape, shards, smallest, top_value):
    factor_of = 1.0
    for dim, shards_of in shards:
        heights = jax.random.uniform(jax.random.fold_in(jax.random.fold_in(own_key, 6), dim), (shards_of,), jnp.float32, smallest / len(shards), top_value / len(shards))
        factor_of = factor_of * jnp.repeat(jnp.exp(heights), shape[dim] // shards_of).reshape((-1,) + (1,) * (len(shape) - 1 - dim))
    return factor_of


def gaussian(key, dims, scale, most, split=(), dtype=jnp.bfloat16):
    entries = jax.random.normal(key, dims, jnp.float32) * scale
    if len(split) > 0:
        entries = steps_of(key, dims, split, -0.22, 0.18) * entries
    return jnp.clip(entries, min=-most, max=most).astype(dtype)


def setup_inputs(seed: int = 0) -> dict:
    key_of = jax.random.split(jax.random.key(seed), 8)
    pole_values = draw_pole_values(jax.random.fold_in(key_of[7], 71), 0)
    weights = jnp.clip(jnp.exp(math.log(0.5) - 1.2039728 * jax.random.uniform(key_of[1], (N,), jnp.float32) ** steps_of(key_of[1], (N,), ((0, 16),), -0.2, 0.2)), 0.15, 0.5)
    centers = draw_centers(jax.random.fold_in(key_of[7], 71), 0)
    offsets = jnp.clip(jax.random.uniform(key_of[3], (N,), jnp.float32, -0.1, 0.1) * steps_of(key_of[3], (N,), ((0, 8),), -0.4, 0.0), -0.1, 0.1)
    chosen = plant(jax.random.randint(key_of[4], (K,), 0, N), jax.random.fold_in(key_of[4], 1), 0, N - 1).astype(jnp.int32)
    column_pole = draw_column_pole(jax.random.fold_in(key_of[7], 71), 0)
    eigen_blocks = gaussian(key_of[6], (QROWS, 2, H), 1.0, 6.0, ((0, 8), (2, 16)))
    return {"pole_values": pole_values, "weights": weights, "centers": centers, "offsets": offsets, "chosen": chosen, "column_pole": column_pole, "eigen_blocks": eigen_blocks}


def block_sums(pole_vals, weight_sq, center_vals, offset_vals, block_rows):
    root_count = center_vals.shape[0]
    block_rows = min(block_rows, root_count)
    center_blocks = center_vals.reshape(root_count // block_rows, block_rows)
    offset_blocks = offset_vals.reshape(root_count // block_rows, block_rows)

    def per_block(blocks):
        distance = pole_vals[None, :] - blocks[0][:, None] - blocks[1][:, None]
        inverse = 1.0 / distance
        weighted = weight_sq[None, :] * inverse
        return (lax.optimization_barrier(jnp.sum(weighted, axis=1)), lax.optimization_barrier(jnp.sum(weighted * inverse, axis=1)), lax.optimization_barrier(jnp.min(jnp.abs(distance), axis=1)))
    sums = lax.map(per_block, (center_blocks, offset_blocks))
    return tuple((item.reshape(root_count) for item in sums))

def newton_update(offset_now, sum_inverse, sum_square, nearest):
    limit = 0.5 * nearest
    return offset_now - jnp.clip((1.0 + sum_inverse) / sum_square, -limit, limit)

def cauchy_block(pole_picked, weight_picked, panel_center, panel_offset, inv_norm):
    distance = pole_picked[:, None] - panel_center[None, :] - panel_offset[None, :]
    return (weight_picked[:, None] * (1.0 / distance) * inv_norm[None, :]).astype(jnp.bfloat16)

def reference(pole_values, weights, centers, offsets, chosen, column_pole, eigen_blocks):
    weight_sq = weights * weights
    offset_now = offsets
    for iteration in range(ITERS):
        sum_inverse, sum_square, nearest = block_sums(pole_values, weight_sq, centers, offset_now, 128)
        offset_now = newton_update(offset_now, sum_inverse, sum_square, nearest)
    panel_center = centers[chosen]
    panel_offset = offset_now[chosen]
    norm_sq = block_sums(pole_values, weight_sq, panel_center, panel_offset, 64)[1]
    inv_norm = lax.rsqrt(norm_sq)
    halves_out = []
    for half_index in range(2):
        pole_index = column_pole[half_index]
        cauchy = cauchy_block(pole_values[pole_index], weights[pole_index], panel_center, panel_offset, inv_norm)
        halves_out.append(jnp.dot(eigen_blocks[:, half_index, :], cauchy, preferred_element_type=jnp.float32))
    return (offset_now, jnp.stack(halves_out, axis=1))
```

```python
import functools

import jax
import jax.numpy as jnp
from jax import lax
from jax.experimental import pallas as pl
from jax.experimental.pallas import tpu as pltpu
from jax.sharding import PartitionSpec as P

MESH = pl.DeviceIdType.MESH
VMEM = pltpu.VMEM
F32 = jnp.float32
BF16 = jnp.bfloat16
ROWS, COLS = 16, 8
N = 65536
TILES = N // 128
PANEL = 2048
MINE = 16
ITERS = 3


def vmem():
    return pl.BlockSpec(memory_space=VMEM)


def greet(row, col):
    barrier = pltpu.get_barrier_semaphore()
    for j in range(1, ROWS):
        pl.semaphore_signal(barrier, inc=1, device_id={"row": lax.rem(row + j, ROWS)}, device_id_type=MESH)
    for j in range(1, COLS):
        pl.semaphore_signal(barrier, inc=1, device_id={"col": lax.rem(col + j, COLS)}, device_id_type=MESH)
    pl.semaphore_wait(barrier, ROWS + COLS - 2)


def spread(src, dst, axis, size, me, send, recv):
    out = []
    for j in range(1, size):
        copy = pltpu.make_async_remote_copy(
            src_ref=src,
            dst_ref=dst.at[me],
            send_sem=send.at[j - 1],
            recv_sem=recv.at[j - 1],
            device_id={axis: lax.rem(me + j, size)},
            device_id_type=MESH,
        )
        copy.start()
        out.append(copy)
    return out


def collect(copies, src, dst, axis, size, me, send, recv):
    for j, copy in enumerate(copies, 1):
        got = pltpu.make_async_remote_copy(
            src_ref=src,
            dst_ref=dst.at[lax.rem(me + size - j, size)],
            send_sem=send.at[j - 1],
            recv_sem=recv.at[j - 1],
            device_id={axis: lax.rem(me + j, size)},
            device_id_type=MESH,
        )
        got.wait_recv()
        copy.wait_send()


def gather_kernel(p_ref, w_ref, o_ref, p_out, w_out, o_out, ps, pr, ws, wr, os_, or_, ls):
    row, col = lax.axis_index("row"), lax.axis_index("col")
    own = [
        pltpu.make_async_copy(p_ref, p_out.at[row], ls.at[0]),
        pltpu.make_async_copy(w_ref, w_out.at[row], ls.at[1]),
        pltpu.make_async_copy(o_ref, o_out.at[col], ls.at[2]),
    ]
    for c in own:
        c.start()
    greet(row, col)
    a = spread(p_ref, p_out, "row", ROWS, row, ps, pr)
    b = spread(w_ref, w_out, "row", ROWS, row, ws, wr)
    c = spread(o_ref, o_out, "col", COLS, col, os_, or_)
    collect(a, p_ref, p_out, "row", ROWS, row, ps, pr)
    collect(b, w_ref, w_out, "row", ROWS, row, ws, wr)
    collect(c, o_ref, o_out, "col", COLS, col, os_, or_)
    for c in own:
        c.wait()


def dma(n):
    return pltpu.SemaphoreType.DMA((n,))


def gather_all(poles, weights, offsets):
    return pl.pallas_call(
        gather_kernel,
        name="gather_all",
        out_shape=(
            jax.ShapeDtypeStruct((ROWS, 32, 128), F32),
            jax.ShapeDtypeStruct((ROWS, 32, 128), F32),
            jax.ShapeDtypeStruct((COLS, 64, 128), F32),
        ),
        in_specs=[vmem()] * 3,
        out_specs=(vmem(),) * 3,
        scratch_shapes=[dma(15), dma(15), dma(15), dma(15), dma(7), dma(7), dma(3)],
        compiler_params=pltpu.CompilerParams(collective_id=0, has_side_effects=True),
    )(poles.reshape(32, 128), weights.reshape(32, 128), offsets.reshape(64, 128))


def limited(t, s1, s2, nearest):
    limit = 0.5 * nearest
    return t - jnp.clip((1.0 + s1) / s2, -limit, limit)


def pieces(x):
    hi = x.astype(BF16)
    rest = x - hi.astype(F32)
    mid = rest.astype(BF16)
    low = (rest - mid.astype(F32)).astype(BF16)
    return hi, mid, low


def panel_roots_kernel(ch_ref, p_ref, w_ref, off_ref, cp_ref, tbl_ref, pw_ref, w2, sp, sq, st, sl):
    row, col = lax.axis_index("row"), lax.axis_index("col")
    dev = row * COLS + col
    lane = lax.broadcasted_iota(jnp.int32, (1, 128), 1)
    w2[...] = w_ref[...] * w_ref[...]
    for i in range(MINE):
        r = ch_ref[i * 128 + dev]
        r1 = jnp.minimum(r + 1, N - 1)
        sp[i : i + 1, :] = jnp.where(lane == (r & 127), p_ref[pl.ds(r >> 7, 1), :], 0.0)
        sq[i : i + 1, :] = jnp.where(lane == (r1 & 127), p_ref[pl.ds(r1 >> 7, 1), :], 0.0)
        st[i : i + 1, :] = jnp.where(lane == (r & 127), off_ref[pl.ds(r >> 7, 1), :], 0.0)
        sl[i : i + 1, :] = jnp.broadcast_to(jnp.where(r == N - 1, 1.0, 0.0), (1, 128))

    def wide(ref):
        return jnp.broadcast_to(jnp.sum(ref[...], axis=1, keepdims=True), (MINE, 128))

    p0, p1, t = wide(sp), wide(sq), wide(st)
    last = sl[...] > 0.5
    c = jnp.where(last, p0 + 0.5, 0.5 * (p0 + p1))
    h = c - p0

    def sums(t):
        def step(s, carry):
            s1, s2 = carry
            for k in range(8):
                pole = p_ref[pl.ds(s * 8 + k, 1), :]
                wsq = w2[pl.ds(s * 8 + k, 1), :]
                inverse = 1.0 / ((pole - c) - t)
                weighted = wsq * inverse
                s1 = s1 + weighted
                s2 = s2 + weighted * inverse
            return s1, s2

        zero = jnp.zeros((MINE, 128), F32)
        s1, s2 = lax.fori_loop(0, TILES // 8, step, (zero, zero))
        return (
            jnp.broadcast_to(jnp.sum(s1, axis=1, keepdims=True), (MINE, 128)),
            jnp.broadcast_to(jnp.sum(s2, axis=1, keepdims=True), (MINE, 128)),
        )

    def iteration(_, t):
        s1, s2 = sums(t)
        left, right = jnp.abs(-h - t), jnp.abs(h - t)
        nearest = jnp.where(last, left, jnp.minimum(left, right))
        return limited(t, s1, s2, nearest)

    t = lax.fori_loop(0, ITERS, iteration, t)
    norm = lax.rsqrt(sums(t)[1])
    index = lax.broadcasted_iota(jnp.int32, (MINE, 128), 0)
    lanes = lax.broadcasted_iota(jnp.int32, (MINE, 128), 1)
    out = jnp.where(lanes == index, c, 0.0)
    out = out + jnp.where(lanes == index + 16, t, 0.0)
    out = out + jnp.where(lanes == index + 32, norm, 0.0)
    tbl_ref[...] = jnp.sum(out, axis=0, keepdims=True)

    table = jnp.concatenate([*pieces(p_ref[...]), *pieces(w_ref[...])], axis=1)
    half = lax.div(col, 4)
    first = lax.rem(col, 4) * 512
    for q in range(4):
        both = cp_ref[:, pl.ds(pl.multiple_of(first + q * 128, 128), 128)]
        idx = jnp.where(half == 0, both[0:1, :], both[1:2, :])
        tile = lax.broadcasted_iota(jnp.int32, (TILES, 128), 0)
        onehot = jnp.where(tile == (idx >> 7), 1.0, 0.0).astype(BF16)
        got = lax.dot_general(table, onehot, (((0,), (0,)), ((), ())), preferred_element_type=F32)
        pick = lax.broadcasted_iota(jnp.int32, (128, 128), 0) == (idx & 127)
        for what in range(2):
            full = got[what * 384 : what * 384 + 128]
            full = full + got[what * 384 + 128 : what * 384 + 256]
            full = full + got[what * 384 + 256 : what * 384 + 384]
            pw_ref[what * 4 + q : what * 4 + q + 1, :] = jnp.sum(
                jnp.where(pick, full, 0.0), axis=0, keepdims=True
            )


def panel_roots(chosen, poles, weights, offsets, column_pole):
    return pl.pallas_call(
        panel_roots_kernel,
        name="panel_roots",
        out_shape=(jax.ShapeDtypeStruct((1, 128), F32), jax.ShapeDtypeStruct((8, 128), F32)),
        in_specs=[pl.BlockSpec(memory_space=pltpu.SMEM)] + [vmem()] * 4,
        out_specs=(vmem(),) * 2,
        scratch_shapes=[VMEM((TILES, 128), F32)] + [VMEM((MINE, 128), F32)] * 4,
        cost_estimate=pl.CostEstimate(flops=30_000_000, bytes_accessed=1 << 20, transcendentals=4_000_000),
    )(chosen, poles, weights, offsets, column_pole)


def share_kernel(tbl_ref, pw_ref, all_tbl, all_pw, mine, ts, tr, ws, wr, us, ur, ls):
    row, col = lax.axis_index("row"), lax.axis_index("col")
    own = [
        pltpu.make_async_copy(tbl_ref, mine.at[col], ls.at[0]),
        pltpu.make_async_copy(pw_ref, all_pw.at[col], ls.at[1]),
    ]
    for c in own:
        c.start()
    greet(row, col)
    a = spread(tbl_ref, mine, "col", COLS, col, ts, tr)
    b = spread(pw_ref, all_pw, "col", COLS, col, ws, wr)
    own[0].wait()
    collect(a, tbl_ref, mine, "col", COLS, col, ts, tr)
    last = pltpu.make_async_copy(mine, all_tbl.at[row], ls.at[2])
    last.start()
    c = spread(mine, all_tbl, "row", ROWS, row, us, ur)
    collect(b, pw_ref, all_pw, "col", COLS, col, ws, wr)
    own[1].wait()
    collect(c, mine, all_tbl, "row", ROWS, row, us, ur)
    last.wait()


def share(tbl, pw):
    return pl.pallas_call(
        share_kernel,
        name="share",
        out_shape=(
            jax.ShapeDtypeStruct((ROWS, COLS, 1, 128), F32),
            jax.ShapeDtypeStruct((COLS, 8, 128), F32),
        ),
        in_specs=[vmem()] * 2,
        out_specs=(vmem(),) * 2,
        scratch_shapes=[VMEM((COLS, 1, 128), F32), dma(7), dma(7), dma(7), dma(7), dma(15), dma(15), dma(3)],
        compiler_params=pltpu.CompilerParams(collective_id=1, has_side_effects=True),
    )(tbl, pw)


KB = 256


def product_kernel(tbl_ref, pw_ref, e_ref, *refs):
    outs, (cauchy, acc) = refs[:8], refs[8:]
    row = lax.axis_index("row")
    z, x = lax.div(row, 4), lax.rem(row, 4)
    half, block = pl.program_id(0), pl.program_id(1)
    lanes = lax.broadcasted_iota(jnp.int32, (128, 128), 1)

    def column(which):
        picked = jnp.where(lanes == which, tbl_ref[...], 0.0)
        return jnp.broadcast_to(jnp.sum(picked, axis=1, keepdims=True), (128, 128))

    for sub in range(KB // 128):
        k = block * (KB // 128) + sub
        center, offset, norm = column(k), column(16 + k), column(32 + k)
        for tile in range(16):
            pole = pw_ref[half * 4 + tile // 4, tile % 4 : tile % 4 + 1, :]
            weight = pw_ref[half * 4 + tile // 4, 4 + tile % 4 : 5 + tile % 4, :]
            inverse = 1.0 / ((pole - center) - offset)
            cauchy[sub * 128 : sub * 128 + 128, tile * 128 : tile * 128 + 128] = (
                (weight * inverse) * norm
            ).astype(BF16)
    acc[...] = lax.dot_general(
        e_ref[0], cauchy[...], (((1,), (1,)), ((), ())), preferred_element_type=F32
    )

    @pl.when(half == 0)
    def _():
        for j in range(4):
            to = lax.rem(z + j, 4)
            outs[j][...] = acc[pl.ds(pl.multiple_of(to * 192, 192), 192), :].astype(outs[j].dtype)

    @pl.when(half == 1)
    def _():
        for j in range(4):
            to = lax.rem(x + j, 4)
            for s in range(4):
                outs[4 + j][s * 48 : s * 48 + 48, :] = acc[
                    pl.ds(pl.multiple_of(s * 192 + to * 48, 48), 48), :
                ].astype(outs[4 + j].dtype)


def product(tbl, pw, halves):
    steps = PANEL // KB

    def first(h, k):
        return (0, jnp.where(h == 0, k, steps - 1))

    def second(h, k):
        return (0, jnp.where(h == 0, 0, k))

    kinds = [F32, BF16, BF16, BF16] * 2
    return pl.pallas_call(
        product_kernel,
        name="product",
        grid=(2, steps),
        out_shape=tuple(jax.ShapeDtypeStruct((192, PANEL), k) for k in kinds),
        in_specs=[
            pl.BlockSpec((128, 128), lambda h, k: (0, 0)),
            pl.BlockSpec((COLS, 8, 128), lambda h, k: (0, 0, 0)),
            pl.BlockSpec((1, 768, 2048), lambda h, k: (h, 0, 0)),
        ],
        out_specs=tuple([pl.BlockSpec((192, KB), first)] * 4 + [pl.BlockSpec((192, KB), second)] * 4),
        scratch_shapes=[VMEM((KB, 2048), BF16), VMEM((768, KB), F32)],
        cost_estimate=pl.CostEstimate(flops=13_000_000_000, bytes_accessed=20 << 20, transcendentals=8_000_000),
    )(tbl, pw, halves)


SUB = 64


def roots_kernel(p_ref, w_ref, c_ref, t_ref, out_ref, w2, pd, xs, a1, a2):
    row, col = lax.axis_index("row"), lax.axis_index("col")
    first = col * 64 + row * 4
    w2[...] = w_ref[...] * w_ref[...]
    lane = lax.broadcasted_iota(jnp.int32, (1, 128), 1)

    def block(b, _):
        c, t = c_ref[pl.ds(b, 1), :], t_ref[pl.ds(b, 1), :]
        own = p_ref[pl.ds(first + b, 1), :]
        origin = own[:, 64:65]
        pd[...] = p_ref[...] - origin
        x = (c - origin) + t
        xs[...] = jnp.broadcast_to(x, (128, 128)).T
        for sub in range(128 // SUB):
            x_sub = xs[sub * SUB : sub * SUB + SUB, :]

            def step(s, carry):
                s1, s2 = carry
                for k in range(4):
                    pole = pd[pl.ds(s * 4 + k, 1), :]
                    wsq = w2[pl.ds(s * 4 + k, 1), :]
                    inverse = 1.0 / (pole - x_sub)
                    weighted = wsq * inverse
                    s1 = s1 + weighted
                    s2 = s2 + weighted * inverse
                return s1, s2

            zero = jnp.zeros((SUB, 128), F32)
            s1, s2 = lax.fori_loop(0, TILES // 4, step, (zero, zero))
            a1[sub * SUB : sub * SUB + SUB, :] = s1
            a2[sub * SUB : sub * SUB + SUB, :] = s2
        s1 = jnp.sum(a1[...].T, axis=0, keepdims=True)
        s2 = jnp.sum(a2[...].T, axis=0, keepdims=True)
        h = c - own
        left, right = jnp.abs(-h - t), jnp.abs(h - t)
        last = (first + b) * 128 + lane == N - 1
        nearest = jnp.where(last, left, jnp.minimum(left, right))
        out_ref[pl.ds(b, 1), :] = limited(t, s1, s2, nearest)
        return 0

    lax.fori_loop(0, 4, block, 0)


def roots(poles, weights, centers, offsets):
    return pl.pallas_call(
        roots_kernel,
        name="roots",
        out_shape=jax.ShapeDtypeStruct((4, 128), F32),
        in_specs=[vmem()] * 4,
        out_specs=vmem(),
        scratch_shapes=[VMEM((TILES, 128), F32)] * 2 + [VMEM((128, 128), F32)] * 3,
        cost_estimate=pl.CostEstimate(flops=25_000_000_000, bytes_accessed=1 << 20, transcendentals=33_000_000),
    )(poles, weights, centers, offsets)


def finish_kernel(t_ref, out_ref, ts, tr, ls):
    row = lax.axis_index("row")
    own = pltpu.make_async_copy(t_ref, out_ref.at[row], ls.at[0])
    own.start()
    barrier = pltpu.get_barrier_semaphore()
    for j in range(1, ROWS):
        pl.semaphore_signal(barrier, inc=1, device_id={"row": lax.rem(row + j, ROWS)}, device_id_type=MESH)
    pl.semaphore_wait(barrier, ROWS - 1)
    a = spread(t_ref, out_ref, "row", ROWS, row, ts, tr)
    collect(a, t_ref, out_ref, "row", ROWS, row, ts, tr)
    own.wait()


def finish(t):
    return pl.pallas_call(
        finish_kernel,
        name="finish",
        out_shape=jax.ShapeDtypeStruct((ROWS, 4, 128), F32),
        in_specs=[vmem()],
        out_specs=vmem(),
        scratch_shapes=[dma(15), dma(15), dma(1)],
        compiler_params=pltpu.CompilerParams(collective_id=2, has_side_effects=True),
    )(t)


def along(j, first):
    pairs = []
    for z in range(4):
        for x in range(4):
            to = ((z + j) % 4, x) if first else (z, (x + j) % 4)
            pairs.append((z * 4 + x, to[0] * 4 + to[1]))
    return pairs


def on_device(pole_values, weights, centers, offsets, chosen, column_pole, eigen_blocks):
    row = lax.axis_index("row")
    z, x = lax.div(row, 4), lax.rem(row, 4)
    all_p, all_w, all_o = gather_all(pole_values, weights, offsets)
    all_p, all_w, all_o = (a.reshape(TILES, 128) for a in (all_p, all_w, all_o))
    tbl, pw = share(*panel_roots(chosen, all_p, all_w, all_o, column_pole))
    halves = jnp.transpose(eigen_blocks, (1, 0, 2))
    blocks = product(tbl.reshape(128, 128), pw, halves)

    def moved(block, j, first):
        return lax.ppermute(block, "row", along(j, first))

    got = [[moved(blocks[4 * half + j], j, half == 0) for j in (1, 2, 3)] for half in range(2)]

    my_centers = lax.dynamic_slice_in_dim(centers.reshape(64, 128), row * 4, 4)
    t = lax.dynamic_slice_in_dim(offsets.reshape(64, 128), row * 4, 4)
    t, blocks = lax.optimization_barrier((t, blocks))
    t = roots(all_p, all_w, my_centers, t)
    t = roots(all_p, all_w, my_centers, t)
    got, t = lax.optimization_barrier((got, t))
    panels, sent = [], []
    for half in range(2):
        total = blocks[4 * half]
        for g in got[half]:
            total = total + g.astype(F32)
        total = total.reshape(4, 48, PANEL)
        me = x if half == 0 else z
        sent.append([
            moved(lax.dynamic_index_in_dim(total, lax.rem(me + j, 4), 0, False).astype(BF16), j, half == 1)
            for j in (1, 2, 3)
        ])
        panels.append(lax.dynamic_index_in_dim(total, me, 0, False))
    t = roots(all_p, all_w, my_centers, t)
    sent, t = lax.optimization_barrier((sent, t))
    offset_now = finish(t).reshape(8192)
    for half in range(2):
        for g in sent[half]:
            panels[half] = panels[half] + g.astype(F32)
    return offset_now, jnp.stack(panels, axis=1)


def solution(mesh):
    placed = (P("row"), P("row"), P("col"), P("col"), P(), P(None, "row"), P("col", None, "row"))
    return jax.shard_map(
        on_device,
        mesh=mesh,
        in_specs=placed,
        out_specs=(P("col"), P(("col", "row"), None, None)),
        check_vma=False,
    )
```

```python
import functools

import jax
import jax.numpy as jnp
from jax import lax
from jax.experimental import pallas as pl
from jax.experimental.pallas import tpu as pltpu
from jax.sharding import PartitionSpec as P

MESH = pl.DeviceIdType.MESH
VMEM = pltpu.VMEM
F32 = jnp.float32
BF16 = jnp.bfloat16
ROWS, COLS = 16, 8
N = 65536
TILES = N // 128
PANEL = 2048
MINE = 16
ITERS = 3


def vmem():
    return pl.BlockSpec(memory_space=VMEM)


def greet(row, col):
    barrier = pltpu.get_barrier_semaphore()
    for j in range(1, ROWS):
        pl.semaphore_signal(barrier, inc=1, device_id={"row": lax.rem(row + j, ROWS)}, device_id_type=MESH)
    for j in range(1, COLS):
        pl.semaphore_signal(barrier, inc=1, device_id={"col": lax.rem(col + j, COLS)}, device_id_type=MESH)
    pl.semaphore_wait(barrier, ROWS + COLS - 2)


def spread(src, dst, axis, size, me, send, recv):
    out = []
    for j in range(1, size):
        copy = pltpu.make_async_remote_copy(
            src_ref=src,
            dst_ref=dst.at[me],
            send_sem=send.at[j - 1],
            recv_sem=recv.at[j - 1],
            device_id={axis: lax.rem(me + j, size)},
            device_id_type=MESH,
        )
        copy.start()
        out.append(copy)
    return out


def collect(copies, src, dst, axis, size, me, send, recv):
    for j, copy in enumerate(copies, 1):
        got = pltpu.make_async_remote_copy(
            src_ref=src,
            dst_ref=dst.at[lax.rem(me + size - j, size)],
            send_sem=send.at[j - 1],
            recv_sem=recv.at[j - 1],
            device_id={axis: lax.rem(me + j, size)},
            device_id_type=MESH,
        )
        got.wait_recv()
        copy.wait_send()


def gather_kernel(p_ref, w_ref, o_ref, p_out, w_out, o_out, ps, pr, ws, wr, os_, or_, ls):
    row, col = lax.axis_index("row"), lax.axis_index("col")
    own = [
        pltpu.make_async_copy(p_ref, p_out.at[row], ls.at[0]),
        pltpu.make_async_copy(w_ref, w_out.at[row], ls.at[1]),
        pltpu.make_async_copy(o_ref, o_out.at[col], ls.at[2]),
    ]
    for c in own:
        c.start()
    greet(row, col)
    a = spread(p_ref, p_out, "row", ROWS, row, ps, pr)
    b = spread(w_ref, w_out, "row", ROWS, row, ws, wr)
    c = spread(o_ref, o_out, "col", COLS, col, os_, or_)
    collect(a, p_ref, p_out, "row", ROWS, row, ps, pr)
    collect(b, w_ref, w_out, "row", ROWS, row, ws, wr)
    collect(c, o_ref, o_out, "col", COLS, col, os_, or_)
    for c in own:
        c.wait()


def dma(n):
    return pltpu.SemaphoreType.DMA((n,))


def gather_all(poles, weights, offsets):
    return pl.pallas_call(
        gather_kernel,
        name="gather_all",
        out_shape=(
            jax.ShapeDtypeStruct((ROWS, 32, 128), F32),
            jax.ShapeDtypeStruct((ROWS, 32, 128), F32),
            jax.ShapeDtypeStruct((COLS, 64, 128), F32),
        ),
        in_specs=[vmem()] * 3,
        out_specs=(vmem(),) * 3,
        scratch_shapes=[dma(15), dma(15), dma(15), dma(15), dma(7), dma(7), dma(3)],
        compiler_params=pltpu.CompilerParams(collective_id=0, has_side_effects=True),
    )(poles.reshape(32, 128), weights.reshape(32, 128), offsets.reshape(64, 128))


def limited(t, s1, s2, nearest):
    limit = 0.5 * nearest
    return t - jnp.clip((1.0 + s1) / s2, -limit, limit)


def pieces(x):
    hi = x.astype(BF16)
    rest = x - hi.astype(F32)
    mid = rest.astype(BF16)
    low = (rest - mid.astype(F32)).astype(BF16)
    return hi, mid, low


def panel_roots_kernel(ch_ref, p_ref, w_ref, off_ref, cp_ref, tbl_ref, pw_ref, w2, sp, sq, st, sl):
    row, col = lax.axis_index("row"), lax.axis_index("col")
    dev = row * COLS + col
    lane = lax.broadcasted_iota(jnp.int32, (1, 128), 1)
    w2[...] = w_ref[...] * w_ref[...]
    for i in range(MINE):
        r = ch_ref[i * 128 + dev]
        r1 = jnp.minimum(r + 1, N - 1)
        sp[i : i + 1, :] = jnp.where(lane == (r & 127), p_ref[pl.ds(r >> 7, 1), :], 0.0)
        sq[i : i + 1, :] = jnp.where(lane == (r1 & 127), p_ref[pl.ds(r1 >> 7, 1), :], 0.0)
        st[i : i + 1, :] = jnp.where(lane == (r & 127), off_ref[pl.ds(r >> 7, 1), :], 0.0)
        sl[i : i + 1, :] = jnp.broadcast_to(jnp.where(r == N - 1, 1.0, 0.0), (1, 128))

    def wide(ref):
        return jnp.broadcast_to(jnp.sum(ref[...], axis=1, keepdims=True), (MINE, 128))

    p0, p1, t = wide(sp), wide(sq), wide(st)
    last = sl[...] > 0.5
    c = jnp.where(last, p0 + 0.5, 0.5 * (p0 + p1))
    h = c - p0

    def sums(t):
        def step(s, carry):
            s1, s2 = carry
            for k in range(8):
                pole = p_ref[pl.ds(s * 8 + k, 1), :]
                wsq = w2[pl.ds(s * 8 + k, 1), :]
                inverse = 1.0 / ((pole - c) - t)
                weighted = wsq * inverse
                s1 = s1 + weighted
                s2 = s2 + weighted * inverse
            return s1, s2

        zero = jnp.zeros((MINE, 128), F32)
        s1, s2 = lax.fori_loop(0, TILES // 8, step, (zero, zero))
        return (
            jnp.broadcast_to(jnp.sum(s1, axis=1, keepdims=True), (MINE, 128)),
            jnp.broadcast_to(jnp.sum(s2, axis=1, keepdims=True), (MINE, 128)),
        )

    def iteration(_, t):
        s1, s2 = sums(t)
        left, right = jnp.abs(-h - t), jnp.abs(h - t)
        nearest = jnp.where(last, left, jnp.minimum(left, right))
        return limited(t, s1, s2, nearest)

    t = lax.fori_loop(0, ITERS, iteration, t)
    norm = lax.rsqrt(sums(t)[1])
    index = lax.broadcasted_iota(jnp.int32, (MINE, 128), 0)
    lanes = lax.broadcasted_iota(jnp.int32, (MINE, 128), 1)
    out = jnp.where(lanes == index, c, 0.0)
    out = out + jnp.where(lanes == index + 16, t, 0.0)
    out = out + jnp.where(lanes == index + 32, norm, 0.0)
    tbl_ref[...] = jnp.sum(out, axis=0, keepdims=True)

    table = jnp.concatenate([*pieces(p_ref[...]), *pieces(w_ref[...])], axis=1)
    half = lax.div(col, 4)
    first = lax.rem(col, 4) * 512
    for q in range(4):
        both = cp_ref[:, pl.ds(pl.multiple_of(first + q * 128, 128), 128)]
        idx = jnp.where(half == 0, both[0:1, :], both[1:2, :])
        tile = lax.broadcasted_iota(jnp.int32, (TILES, 128), 0)
        onehot = jnp.where(tile == (idx >> 7), 1.0, 0.0).astype(BF16)
        got = lax.dot_general(table, onehot, (((0,), (0,)), ((), ())), preferred_element_type=F32)
        pick = lax.broadcasted_iota(jnp.int32, (128, 128), 0) == (idx & 127)
        for what in range(2):
            full = got[what * 384 : what * 384 + 128]
            full = full + got[what * 384 + 128 : what * 384 + 256]
            full = full + got[what * 384 + 256 : what * 384 + 384]
            pw_ref[what * 4 + q : what * 4 + q + 1, :] = jnp.sum(
                jnp.where(pick, full, 0.0), axis=0, keepdims=True
            )


def panel_roots(chosen, poles, weights, offsets, column_pole):
    return pl.pallas_call(
        panel_roots_kernel,
        name="panel_roots",
        out_shape=(jax.ShapeDtypeStruct((1, 128), F32), jax.ShapeDtypeStruct((8, 128), F32)),
        in_specs=[pl.BlockSpec(memory_space=pltpu.SMEM)] + [vmem()] * 4,
        out_specs=(vmem(),) * 2,
        scratch_shapes=[VMEM((TILES, 128), F32)] + [VMEM((MINE, 128), F32)] * 4,
        cost_estimate=pl.CostEstimate(flops=30_000_000, bytes_accessed=1 << 20, transcendentals=4_000_000),
    )(chosen, poles, weights, offsets, column_pole)


def share_kernel(tbl_ref, pw_ref, all_tbl, all_pw, mine, ts, tr, ws, wr, us, ur, ls):
    row, col = lax.axis_index("row"), lax.axis_index("col")
    own = [
        pltpu.make_async_copy(tbl_ref, mine.at[col], ls.at[0]),
        pltpu.make_async_copy(pw_ref, all_pw.at[col], ls.at[1]),
    ]
    for c in own:
        c.start()
    greet(row, col)
    a = spread(tbl_ref, mine, "col", COLS, col, ts, tr)
    b = spread(pw_ref, all_pw, "col", COLS, col, ws, wr)
    own[0].wait()
    collect(a, tbl_ref, mine, "col", COLS, col, ts, tr)
    last = pltpu.make_async_copy(mine, all_tbl.at[row], ls.at[2])
    last.start()
    c = spread(mine, all_tbl, "row", ROWS, row, us, ur)
    collect(b, pw_ref, all_pw, "col", COLS, col, ws, wr)
    own[1].wait()
    collect(c, mine, all_tbl, "row", ROWS, row, us, ur)
    last.wait()


def share(tbl, pw):
    return pl.pallas_call(
        share_kernel,
        name="share",
        out_shape=(
            jax.ShapeDtypeStruct((ROWS, COLS, 1, 128), F32),
            jax.ShapeDtypeStruct((COLS, 8, 128), F32),
        ),
        in_specs=[vmem()] * 2,
        out_specs=(vmem(),) * 2,
        scratch_shapes=[VMEM((COLS, 1, 128), F32), dma(7), dma(7), dma(7), dma(7), dma(15), dma(15), dma(3)],
        compiler_params=pltpu.CompilerParams(collective_id=1, has_side_effects=True),
    )(tbl, pw)


KB = 256


def product_kernel(tbl_ref, pw_ref, e_ref, *refs):
    outs, (cauchy, acc) = refs[:8], refs[8:]
    row = lax.axis_index("row")
    z, x = lax.div(row, 4), lax.rem(row, 4)
    half, block = pl.program_id(0), pl.program_id(1)
    lanes = lax.broadcasted_iota(jnp.int32, (128, 128), 1)

    def column(which):
        picked = jnp.where(lanes == which, tbl_ref[...], 0.0)
        return jnp.broadcast_to(jnp.sum(picked, axis=1, keepdims=True), (128, 128))

    for sub in range(KB // 128):
        k = block * (KB // 128) + sub
        center, offset, norm = column(k), column(16 + k), column(32 + k)
        for tile in range(16):
            pole = pw_ref[half * 4 + tile // 4, tile % 4 : tile % 4 + 1, :]
            weight = pw_ref[half * 4 + tile // 4, 4 + tile % 4 : 5 + tile % 4, :]
            inverse = 1.0 / ((pole - center) - offset)
            cauchy[sub * 128 : sub * 128 + 128, tile * 128 : tile * 128 + 128] = (
                (weight * inverse) * norm
            ).astype(BF16)
    acc[...] = lax.dot_general(
        e_ref[0], cauchy[...], (((1,), (1,)), ((), ())), preferred_element_type=F32
    )

    @pl.when(half == 0)
    def _():
        for j in range(4):
            to = lax.rem(z + j, 4)
            outs[j][...] = acc[pl.ds(pl.multiple_of(to * 192, 192), 192), :].astype(outs[j].dtype)

    @pl.when(half == 1)
    def _():
        for j in range(4):
            to = lax.rem(x + j, 4)
            for s in range(4):
                outs[4 + j][s * 48 : s * 48 + 48, :] = acc[
                    pl.ds(pl.multiple_of(s * 192 + to * 48, 48), 48), :
                ].astype(outs[4 + j].dtype)


def product(tbl, pw, halves):
    steps = PANEL // KB

    def first(h, k):
        return (0, jnp.where(h == 0, k, steps - 1))

    def second(h, k):
        return (0, jnp.where(h == 0, 0, k))

    kinds = [F32, BF16, BF16, BF16] * 2
    return pl.pallas_call(
        product_kernel,
        name="product",
        grid=(2, steps),
        out_shape=tuple(jax.ShapeDtypeStruct((192, PANEL), k) for k in kinds),
        in_specs=[
            pl.BlockSpec((128, 128), lambda h, k: (0, 0)),
            pl.BlockSpec((COLS, 8, 128), lambda h, k: (0, 0, 0)),
            pl.BlockSpec((1, 768, 2048), lambda h, k: (h, 0, 0)),
        ],
        out_specs=tuple([pl.BlockSpec((192, KB), first)] * 4 + [pl.BlockSpec((192, KB), second)] * 4),
        scratch_shapes=[VMEM((KB, 2048), BF16), VMEM((768, KB), F32)],
        cost_estimate=pl.CostEstimate(flops=13_000_000_000, bytes_accessed=20 << 20, transcendentals=8_000_000),
    )(tbl, pw, halves)


CHAIN = 64
WINDOW = 5
PAIRS = TILES // 2


def weight_tables(w_ref, q):
    w = jnp.concatenate([w_ref[pl.ds(2 * q, 1), :], w_ref[pl.ds(2 * q + 1, 1), :]], axis=1)
    w = jnp.broadcast_to(w, (8, 256))
    first = w.astype(BF16)
    exact = w * w / first.astype(F32)
    lane = lax.broadcasted_iota(jnp.int32, (8, 256), 1)
    turn = lax.rem(lane * 79 + 37, 128).astype(F32) / 128.0 + (1.0 / 256.0 - 0.5)
    step = jnp.where(exact >= 0.25, 2.0**-9, 2.0**-10)
    return first, (exact + turn * step).astype(BF16)


def root_block(b, first, p_ref, w_ref, c_ref, t_ref, out_ref, wa, wv, pd, pb, xs, a1, a2):
    lane = lax.broadcasted_iota(jnp.int32, (1, 128), 1)
    c = c_ref[pl.ds(b, 1), :]
    own = p_ref[pl.ds(first + b, 1), :]
    origin = own[:, 64:65]
    start = jnp.clip(lax.div(first + b, 2) - WINDOW // 2, 0, PAIRS - WINDOW)
    pd[...] = p_ref[...] - origin

    def fill(q, _):
        pole = jnp.concatenate([pd[pl.ds(2 * q, 1), :], pd[pl.ds(2 * q + 1, 1), :]], axis=1)
        pb[q] = jnp.broadcast_to(pole, (8, 256)).astype(BF16)
        return 0

    lax.fori_loop(0, PAIRS, fill, 0, unroll=8)
    for k in range(WINDOW):
        wa[start + k] = jnp.zeros((8, 256), BF16)
        wv[start + k] = jnp.zeros((8, 256), BF16)
        pb[start + k] = jnp.full((8, 256), 8192.0, BF16)
    one = jnp.ones((8, 256), BF16)
    h = c - own
    last = (first + b) * 128 + lane == N - 1

    def iteration(_, t):
        xs[...] = jnp.broadcast_to((c - origin) + t, (128, 128)).T

        def groups(g, _):
            x_g = [xs[pl.ds(pl.multiple_of(g * 16 + 8 * k, 8), 8), :] for k in range(2)]
            x_w = [jnp.concatenate([v, v], axis=1).astype(BF16) for v in x_g]

            def chain(s, carry):
                sums = [[None, None], [None, None]]

                def add(k, scaled, v):
                    one_ = scaled.astype(F32) * v.astype(F32)
                    two_ = scaled.astype(F32) * scaled.astype(F32)
                    sums[k][0] = one_ if sums[k][0] is None else sums[k][0] + one_
                    sums[k][1] = two_ if sums[k][1] is None else sums[k][1] + two_

                for i in range(0, CHAIN, 2):
                    q = s * CHAIN + i
                    for k in range(2):
                        a, d = pb[q] - x_w[k], pb[q + 1] - x_w[k]
                        inverse = one / (a * d)
                        add(k, wa[q] * (d * inverse), wv[q])
                        add(k, wa[q + 1] * (a * inverse), wv[q + 1])
                return tuple(tuple(c + s for c, s in zip(cs, ss)) for cs, ss in zip(carry, sums))

            zero = jnp.zeros((8, 256), F32)
            far = lax.fori_loop(0, PAIRS // CHAIN, chain, ((zero, zero), (zero, zero)))
            near = [[f[:, :128] + f[:, 128:] for f in fs] for fs in far]
            for i in range(2 * WINDOW):
                pole = pd[pl.ds(2 * start + i, 1), :]
                w = w_ref[pl.ds(2 * start + i, 1), :]
                wsq = w * w
                for k in range(2):
                    inverse = 1.0 / (pole - x_g[k])
                    weighted = wsq * inverse
                    near[k][0] = near[k][0] + weighted
                    near[k][1] = near[k][1] + weighted * inverse
            for k in range(2):
                at = pl.ds(pl.multiple_of(g * 16 + 8 * k, 8), 8)
                a1[at, :], a2[at, :] = near[k]
            return 0

        lax.fori_loop(0, 8, groups, 0)
        s1 = jnp.sum(a1[...].T, axis=0, keepdims=True)
        s2 = jnp.sum(a2[...].T, axis=0, keepdims=True)
        left, right = jnp.abs(-h - t), jnp.abs(h - t)
        nearest = jnp.where(last, left, jnp.minimum(left, right))
        return limited(t, s1, s2, nearest)

    out_ref[pl.ds(b, 1), :] = lax.fori_loop(0, ITERS, iteration, t_ref[pl.ds(b, 1), :])
    for k in range(WINDOW):
        wa[start + k], wv[start + k] = weight_tables(w_ref, start + k)


def roots_kernel(p_ref, w_ref, c_ref, t_ref, out_ref, wa, wv, *scratch):
    row, col = lax.axis_index("row"), lax.axis_index("col")
    first = col * 64 + row * 4 + (4 - t_ref.shape[0]) * FIRST_OF[t_ref.shape[0]]

    def fill(q, _):
        wa[q], wv[q] = weight_tables(w_ref, q)
        return 0

    lax.fori_loop(0, PAIRS, fill, 0, unroll=4)

    def block(b, _):
        root_block(b, first, p_ref, w_ref, c_ref, t_ref, out_ref, wa, wv, *scratch)
        return 0

    lax.fori_loop(0, t_ref.shape[0], block, 0)


FIRST_OF = {3: 0, 1: 1}


def roots(poles, weights, centers, offsets):
    blocks = offsets.shape[0]
    return pl.pallas_call(
        roots_kernel,
        name=f"roots{blocks}",
        out_shape=jax.ShapeDtypeStruct((blocks, 128), F32),
        in_specs=[vmem()] * 4,
        out_specs=vmem(),
        scratch_shapes=[VMEM((PAIRS, 8, 256), BF16)] * 2
        + [VMEM((TILES, 128), F32), VMEM((PAIRS, 8, 256), BF16)]
        + [VMEM((128, 128), F32)] * 3,
        cost_estimate=pl.CostEstimate(
            flops=blocks * 12_000_000_000, bytes_accessed=1 << 20, transcendentals=33_000_000
        ),
    )(poles, weights, centers, offsets)


def finish_kernel(t_ref, out_ref, ts, tr, ls):
    row = lax.axis_index("row")
    own = pltpu.make_async_copy(t_ref, out_ref.at[row], ls.at[0])
    own.start()
    barrier = pltpu.get_barrier_semaphore()
    for j in range(1, ROWS):
        pl.semaphore_signal(barrier, inc=1, device_id={"row": lax.rem(row + j, ROWS)}, device_id_type=MESH)
    pl.semaphore_wait(barrier, ROWS - 1)
    a = spread(t_ref, out_ref, "row", ROWS, row, ts, tr)
    collect(a, t_ref, out_ref, "row", ROWS, row, ts, tr)
    own.wait()


def finish(t):
    return pl.pallas_call(
        finish_kernel,
        name="finish",
        out_shape=jax.ShapeDtypeStruct((ROWS, 4, 128), F32),
        in_specs=[vmem()],
        out_specs=vmem(),
        scratch_shapes=[dma(15), dma(15), dma(1)],
        compiler_params=pltpu.CompilerParams(collective_id=2, has_side_effects=True),
    )(t)


def along(j, first):
    pairs = []
    for z in range(4):
        for x in range(4):
            to = ((z + j) % 4, x) if first else (z, (x + j) % 4)
            pairs.append((z * 4 + x, to[0] * 4 + to[1]))
    return pairs


def on_device(pole_values, weights, centers, offsets, chosen, column_pole, eigen_blocks):
    row = lax.axis_index("row")
    z, x = lax.div(row, 4), lax.rem(row, 4)
    all_p, all_w, all_o = gather_all(pole_values, weights, offsets)
    all_p, all_w, all_o = (a.reshape(TILES, 128) for a in (all_p, all_w, all_o))
    tbl, pw = share(*panel_roots(chosen, all_p, all_w, all_o, column_pole))
    halves = jnp.transpose(eigen_blocks, (1, 0, 2))
    blocks = product(tbl.reshape(128, 128), pw, halves)

    def moved(block, j, first):
        return lax.ppermute(block, "row", along(j, first))

    got = [[moved(blocks[4 * half + j], j, half == 0) for j in (1, 2, 3)] for half in range(2)]

    my_centers = lax.dynamic_slice_in_dim(centers.reshape(64, 128), row * 4, 4)
    t = lax.dynamic_slice_in_dim(offsets.reshape(64, 128), row * 4, 4)
    t, blocks = lax.optimization_barrier((t, blocks))
    t_most = roots(all_p, all_w, my_centers[:3], t[:3])
    got, t_most, t_rest = lax.optimization_barrier((got, t_most, t[3:]))
    panels, sent = [], []
    for half in range(2):
        total = blocks[4 * half]
        for g in got[half]:
            total = total + g.astype(F32)
        total = total.reshape(4, 48, PANEL)
        me = x if half == 0 else z
        sent.append([
            moved(lax.dynamic_index_in_dim(total, lax.rem(me + j, 4), 0, False).astype(BF16), j, half == 1)
            for j in (1, 2, 3)
        ])
        panels.append(lax.dynamic_index_in_dim(total, me, 0, False))
    t = jnp.concatenate([t_most, roots(all_p, all_w, my_centers[3:], t_rest)])
    sent, t = lax.optimization_barrier((sent, t))
    offset_now = finish(t).reshape(8192)
    for half in range(2):
        for g in sent[half]:
            panels[half] = panels[half] + g.astype(F32)
    return offset_now, jnp.stack(panels, axis=1)


def solution(mesh):
    placed = (P("row"), P("row"), P("col"), P("col"), P(), P(None, "row"), P("col", None, "row"))
    return jax.shard_map(
        on_device,
        mesh=mesh,
        in_specs=placed,
        out_specs=(P("col"), P(("col", "row"), None, None)),
        check_vma=False,
    )
```

```python
import jax
import jax.numpy as jnp
from jax import lax
from jax.experimental import pallas as pl
from jax.experimental.pallas import tpu as pltpu
from jax.sharding import PartitionSpec as P

MESH = pl.DeviceIdType.MESH
VMEM = pltpu.VMEM
F32 = jnp.float32
BF16 = jnp.bfloat16
ROWS, COLS = 16, 8
N = 65536
TILES = N // 128
PANEL = 2048
MINE = 16
ITERS = 3


def vmem():
    return pl.BlockSpec(memory_space=VMEM)


def greet(row, col):
    barrier = pltpu.get_barrier_semaphore()
    for j in range(1, ROWS):
        pl.semaphore_signal(barrier, inc=1, device_id={"row": lax.rem(row + j, ROWS)}, device_id_type=MESH)
    for j in range(1, COLS):
        pl.semaphore_signal(barrier, inc=1, device_id={"col": lax.rem(col + j, COLS)}, device_id_type=MESH)
    pl.semaphore_wait(barrier, ROWS + COLS - 2)


def spread(src, dst, axis, size, me, send, recv):
    out = []
    for j in range(1, size):
        copy = pltpu.make_async_remote_copy(
            src_ref=src,
            dst_ref=dst.at[me],
            send_sem=send.at[j - 1],
            recv_sem=recv.at[j - 1],
            device_id={axis: lax.rem(me + j, size)},
            device_id_type=MESH,
        )
        copy.start()
        out.append(copy)
    return out


def collect(copies, src, dst, axis, size, me, send, recv):
    for j, copy in enumerate(copies, 1):
        got = pltpu.make_async_remote_copy(
            src_ref=src,
            dst_ref=dst.at[lax.rem(me + size - j, size)],
            send_sem=send.at[j - 1],
            recv_sem=recv.at[j - 1],
            device_id={axis: lax.rem(me + j, size)},
            device_id_type=MESH,
        )
        got.wait_recv()
        copy.wait_send()


def gather_kernel(p_ref, w_ref, o_ref, p_out, w_out, o_out, ps, pr, ws, wr, os_, or_, ls):
    row, col = lax.axis_index("row"), lax.axis_index("col")
    own = [
        pltpu.make_async_copy(p_ref, p_out.at[row], ls.at[0]),
        pltpu.make_async_copy(w_ref, w_out.at[row], ls.at[1]),
        pltpu.make_async_copy(o_ref, o_out.at[col], ls.at[2]),
    ]
    for c in own:
        c.start()
    greet(row, col)
    a = spread(p_ref, p_out, "row", ROWS, row, ps, pr)
    b = spread(w_ref, w_out, "row", ROWS, row, ws, wr)
    c = spread(o_ref, o_out, "col", COLS, col, os_, or_)
    collect(a, p_ref, p_out, "row", ROWS, row, ps, pr)
    collect(b, w_ref, w_out, "row", ROWS, row, ws, wr)
    collect(c, o_ref, o_out, "col", COLS, col, os_, or_)
    for c in own:
        c.wait()


def dma(n):
    return pltpu.SemaphoreType.DMA((n,))


def gather_all(poles, weights, offsets):
    return pl.pallas_call(
        gather_kernel,
        name="gather_all",
        out_shape=(
            jax.ShapeDtypeStruct((ROWS, 32, 128), F32),
            jax.ShapeDtypeStruct((ROWS, 32, 128), F32),
            jax.ShapeDtypeStruct((COLS, 64, 128), F32),
        ),
        in_specs=[vmem()] * 3,
        out_specs=(vmem(),) * 3,
        scratch_shapes=[dma(15), dma(15), dma(15), dma(15), dma(7), dma(7), dma(3)],
        compiler_params=pltpu.CompilerParams(collective_id=0, has_side_effects=True),
    )(poles.reshape(32, 128), weights.reshape(32, 128), offsets.reshape(64, 128))


def limited(t, s1, s2, nearest):
    limit = 0.5 * nearest
    return t - jnp.clip((1.0 + s1) / s2, -limit, limit)


def pieces(x):
    hi = x.astype(BF16)
    rest = x - hi.astype(F32)
    mid = rest.astype(BF16)
    low = (rest - mid.astype(F32)).astype(BF16)
    return hi, mid, low


def panel_roots_kernel(ch_ref, p_ref, w_ref, off_ref, cp_ref, tbl_ref, pw_ref, w2, sp, sq, st, sl):
    row, col = lax.axis_index("row"), lax.axis_index("col")
    dev = row * COLS + col
    lane = lax.broadcasted_iota(jnp.int32, (1, 128), 1)
    w2[...] = w_ref[...] * w_ref[...]
    for i in range(MINE):
        r = ch_ref[i * 128 + dev]
        r1 = jnp.minimum(r + 1, N - 1)
        sp[i : i + 1, :] = jnp.where(lane == (r & 127), p_ref[pl.ds(r >> 7, 1), :], 0.0)
        sq[i : i + 1, :] = jnp.where(lane == (r1 & 127), p_ref[pl.ds(r1 >> 7, 1), :], 0.0)
        st[i : i + 1, :] = jnp.where(lane == (r & 127), off_ref[pl.ds(r >> 7, 1), :], 0.0)
        sl[i : i + 1, :] = jnp.broadcast_to(jnp.where(r == N - 1, 1.0, 0.0), (1, 128))

    def wide(ref):
        return jnp.broadcast_to(jnp.sum(ref[...], axis=1, keepdims=True), (MINE, 128))

    p0, p1, t = wide(sp), wide(sq), wide(st)
    last = sl[...] > 0.5
    c = jnp.where(last, p0 + 0.5, 0.5 * (p0 + p1))
    h = c - p0

    def sums(t):
        def step(s, carry):
            s1, s2 = carry
            for k in range(8):
                pole = p_ref[pl.ds(s * 8 + k, 1), :]
                wsq = w2[pl.ds(s * 8 + k, 1), :]
                inverse = 1.0 / ((pole - c) - t)
                weighted = wsq * inverse
                s1 = s1 + weighted
                s2 = s2 + weighted * inverse
            return s1, s2

        zero = jnp.zeros((MINE, 128), F32)
        s1, s2 = lax.fori_loop(0, TILES // 8, step, (zero, zero))
        return (
            jnp.broadcast_to(jnp.sum(s1, axis=1, keepdims=True), (MINE, 128)),
            jnp.broadcast_to(jnp.sum(s2, axis=1, keepdims=True), (MINE, 128)),
        )

    def iteration(_, t):
        s1, s2 = sums(t)
        left, right = jnp.abs(-h - t), jnp.abs(h - t)
        nearest = jnp.where(last, left, jnp.minimum(left, right))
        return limited(t, s1, s2, nearest)

    t = lax.fori_loop(0, ITERS, iteration, t)
    norm = lax.rsqrt(sums(t)[1])
    index = lax.broadcasted_iota(jnp.int32, (MINE, 128), 0)
    lanes = lax.broadcasted_iota(jnp.int32, (MINE, 128), 1)
    out = jnp.where(lanes == index, c, 0.0)
    out = out + jnp.where(lanes == index + 16, t, 0.0)
    out = out + jnp.where(lanes == index + 32, norm, 0.0)
    tbl_ref[...] = jnp.sum(out, axis=0, keepdims=True)

    table = jnp.concatenate([*pieces(p_ref[...]), *pieces(w_ref[...])], axis=1)
    half = lax.div(col, 4)
    first = lax.rem(col, 4) * 512
    for q in range(4):
        both = cp_ref[:, pl.ds(pl.multiple_of(first + q * 128, 128), 128)]
        idx = jnp.where(half == 0, both[0:1, :], both[1:2, :])
        tile = lax.broadcasted_iota(jnp.int32, (TILES, 128), 0)
        onehot = jnp.where(tile == (idx >> 7), 1.0, 0.0).astype(BF16)
        got = lax.dot_general(table, onehot, (((0,), (0,)), ((), ())), preferred_element_type=F32)
        pick = lax.broadcasted_iota(jnp.int32, (128, 128), 0) == (idx & 127)
        for what in range(2):
            full = got[what * 384 : what * 384 + 128]
            full = full + got[what * 384 + 128 : what * 384 + 256]
            full = full + got[what * 384 + 256 : what * 384 + 384]
            pw_ref[what * 4 + q : what * 4 + q + 1, :] = jnp.sum(
                jnp.where(pick, full, 0.0), axis=0, keepdims=True
            )


def panel_roots(chosen, poles, weights, offsets, column_pole):
    return pl.pallas_call(
        panel_roots_kernel,
        name="panel_roots",
        out_shape=(jax.ShapeDtypeStruct((1, 128), F32), jax.ShapeDtypeStruct((8, 128), F32)),
        in_specs=[pl.BlockSpec(memory_space=pltpu.SMEM)] + [vmem()] * 4,
        out_specs=(vmem(),) * 2,
        scratch_shapes=[VMEM((TILES, 128), F32)] + [VMEM((MINE, 128), F32)] * 4,
        cost_estimate=pl.CostEstimate(flops=30_000_000, bytes_accessed=1 << 20, transcendentals=4_000_000),
    )(chosen, poles, weights, offsets, column_pole)


def share_kernel(tbl_ref, pw_ref, all_tbl, all_pw, mine, ts, tr, ws, wr, us, ur, ls):
    row, col = lax.axis_index("row"), lax.axis_index("col")
    own = [
        pltpu.make_async_copy(tbl_ref, mine.at[col], ls.at[0]),
        pltpu.make_async_copy(pw_ref, all_pw.at[col], ls.at[1]),
    ]
    for c in own:
        c.start()
    greet(row, col)
    a = spread(tbl_ref, mine, "col", COLS, col, ts, tr)
    b = spread(pw_ref, all_pw, "col", COLS, col, ws, wr)
    own[0].wait()
    collect(a, tbl_ref, mine, "col", COLS, col, ts, tr)
    last = pltpu.make_async_copy(mine, all_tbl.at[row], ls.at[2])
    last.start()
    c = spread(mine, all_tbl, "row", ROWS, row, us, ur)
    collect(b, pw_ref, all_pw, "col", COLS, col, ws, wr)
    own[1].wait()
    collect(c, mine, all_tbl, "row", ROWS, row, us, ur)
    last.wait()


def share(tbl, pw):
    return pl.pallas_call(
        share_kernel,
        name="share",
        out_shape=(
            jax.ShapeDtypeStruct((ROWS, COLS, 1, 128), F32),
            jax.ShapeDtypeStruct((COLS, 8, 128), F32),
        ),
        in_specs=[vmem()] * 2,
        out_specs=(vmem(),) * 2,
        scratch_shapes=[VMEM((COLS, 1, 128), F32), dma(7), dma(7), dma(7), dma(7), dma(15), dma(15), dma(3)],
        compiler_params=pltpu.CompilerParams(collective_id=1, has_side_effects=True),
    )(tbl, pw)


KB = 256


def product_kernel(tbl_ref, pw_ref, e_ref, *refs):
    outs, (cauchy, acc) = refs[:8], refs[8:]
    row = lax.axis_index("row")
    z, x = lax.div(row, 4), lax.rem(row, 4)
    half, block = pl.program_id(0), pl.program_id(1)
    lanes = lax.broadcasted_iota(jnp.int32, (128, 128), 1)

    def column(which):
        picked = jnp.where(lanes == which, tbl_ref[...], 0.0)
        return jnp.broadcast_to(jnp.sum(picked, axis=1, keepdims=True), (128, 128))

    for sub in range(KB // 128):
        k = block * (KB // 128) + sub
        center, offset, norm = column(k), column(16 + k), column(32 + k)
        for tile in range(16):
            pole = pw_ref[half * 4 + tile // 4, tile % 4 : tile % 4 + 1, :]
            weight = pw_ref[half * 4 + tile // 4, 4 + tile % 4 : 5 + tile % 4, :]
            inverse = 1.0 / ((pole - center) - offset)
            cauchy[sub * 128 : sub * 128 + 128, tile * 128 : tile * 128 + 128] = (
                (weight * inverse) * norm
            ).astype(BF16)
    acc[...] = lax.dot_general(
        e_ref[0], cauchy[...], (((1,), (1,)), ((), ())), preferred_element_type=F32
    )

    @pl.when(half == 0)
    def _():
        for j in range(4):
            to = lax.rem(z + j, 4)
            outs[j][...] = acc[pl.ds(pl.multiple_of(to * 192, 192), 192), :].astype(outs[j].dtype)

    @pl.when(half == 1)
    def _():
        for j in range(4):
            to = lax.rem(x + j, 4)
            for s in range(4):
                outs[4 + j][s * 48 : s * 48 + 48, :] = acc[
                    pl.ds(pl.multiple_of(s * 192 + to * 48, 48), 48), :
                ].astype(outs[4 + j].dtype)


def product(tbl, pw, halves):
    steps = PANEL // KB

    def first(h, k):
        return (0, jnp.where(h == 0, k, steps - 1))

    def second(h, k):
        return (0, jnp.where(h == 0, 0, k))

    kinds = [F32, BF16, BF16, BF16] * 2
    return pl.pallas_call(
        product_kernel,
        name="product",
        grid=(2, steps),
        out_shape=tuple(jax.ShapeDtypeStruct((192, PANEL), k) for k in kinds),
        in_specs=[
            pl.BlockSpec((128, 128), lambda h, k: (0, 0)),
            pl.BlockSpec((COLS, 8, 128), lambda h, k: (0, 0, 0)),
            pl.BlockSpec((1, 768, 2048), lambda h, k: (h, 0, 0)),
        ],
        out_specs=tuple([pl.BlockSpec((192, KB), first)] * 4 + [pl.BlockSpec((192, KB), second)] * 4),
        scratch_shapes=[VMEM((KB, 2048), BF16), VMEM((768, KB), F32)],
        cost_estimate=pl.CostEstimate(flops=13_000_000_000, bytes_accessed=20 << 20, transcendentals=8_000_000),
    )(tbl, pw, halves)


CHAIN = 64
WINDOW = 5
PAIRS = TILES // 2


def weight_tables(w_ref, q):
    w = jnp.concatenate([w_ref[pl.ds(2 * q, 1), :], w_ref[pl.ds(2 * q + 1, 1), :]], axis=1)
    w = jnp.broadcast_to(w, (8, 256))
    first = w.astype(BF16)
    exact = w * w / first.astype(F32)
    lane = lax.broadcasted_iota(jnp.int32, (8, 256), 1)
    turn = lax.rem(lane * 79 + 37, 128).astype(F32) / 128.0 + (1.0 / 256.0 - 0.5)
    step = jnp.where(exact >= 0.25, 2.0**-9, 2.0**-10)
    return first, (exact + turn * step).astype(BF16)


def root_block(b, first, local, p_ref, w_ref, c_ref, t_ref, out_ref, wa, wv, pd, pb, xs, a1, a2):
    lane = lax.broadcasted_iota(jnp.int32, (1, 128), 1)
    c = c_ref[pl.ds(local + b, 1), :]
    own = p_ref[pl.ds(first + b, 1), :]
    origin = own[:, 64:65]
    near_rows = [lax.rem(lax.div(first + b, 2) + PAIRS - WINDOW // 2 + k, PAIRS) for k in range(WINDOW)]
    pd[...] = p_ref[...] - origin

    def fill(q, _):
        pole = jnp.concatenate([pd[pl.ds(2 * q, 1), :], pd[pl.ds(2 * q + 1, 1), :]], axis=1)
        pb[q] = jnp.broadcast_to(pole, (8, 256)).astype(BF16)
        return 0

    lax.fori_loop(0, PAIRS, fill, 0, unroll=8)
    for q in near_rows:
        wa[q] = jnp.zeros((8, 256), BF16)
        wv[q] = jnp.zeros((8, 256), BF16)
        pb[q] = jnp.full((8, 256), 8192.0, BF16)
    one = jnp.ones((8, 256), BF16)
    h = c - own
    last = (first + b) * 128 + lane == N - 1

    def iteration(_, t):
        xs[...] = jnp.broadcast_to((c - origin) + t, (128, 128)).T

        def groups(g, _):
            x_g = [xs[pl.ds(pl.multiple_of(g * 16 + 8 * k, 8), 8), :] for k in range(2)]
            x_w = [jnp.concatenate([v, v], axis=1).astype(BF16) for v in x_g]

            def chain(s, carry):
                sums = [[None, None], [None, None]]

                def add(k, scaled, v):
                    one_ = scaled.astype(F32) * v.astype(F32)
                    two_ = scaled.astype(F32) * scaled.astype(F32)
                    sums[k][0] = one_ if sums[k][0] is None else sums[k][0] + one_
                    sums[k][1] = two_ if sums[k][1] is None else sums[k][1] + two_

                for i in range(0, CHAIN, 2):
                    q = s * CHAIN + i
                    for k in range(2):
                        a, d = pb[q] - x_w[k], pb[q + 1] - x_w[k]
                        inverse = one / (a * d)
                        add(k, wa[q] * (d * inverse), wv[q])
                        add(k, wa[q + 1] * (a * inverse), wv[q + 1])
                return tuple(tuple(c + s for c, s in zip(cs, ss)) for cs, ss in zip(carry, sums))

            zero = jnp.zeros((8, 256), F32)
            far = lax.fori_loop(0, PAIRS // CHAIN, chain, ((zero, zero), (zero, zero)))
            near = [[f[:, :128] + f[:, 128:] for f in fs] for fs in far]
            for i in range(2 * WINDOW):
                at = pl.ds(2 * near_rows[i // 2] + i % 2, 1)
                pole = pd[at, :]
                w = w_ref[at, :]
                wsq = w * w
                for k in range(2):
                    inverse = 1.0 / (pole - x_g[k])
                    weighted = wsq * inverse
                    near[k][0] = near[k][0] + weighted
                    near[k][1] = near[k][1] + weighted * inverse
            for k in range(2):
                at = pl.ds(pl.multiple_of(g * 16 + 8 * k, 8), 8)
                a1[at, :], a2[at, :] = near[k]
            return 0

        lax.fori_loop(0, 8, groups, 0)
        s1 = jnp.sum(a1[...].T, axis=0, keepdims=True)
        s2 = jnp.sum(a2[...].T, axis=0, keepdims=True)
        left, right = jnp.abs(-h - t), jnp.abs(h - t)
        nearest = jnp.where(last, left, jnp.minimum(left, right))
        return limited(t, s1, s2, nearest)

    out_ref[pl.ds(b, 1), :] = lax.fori_loop(0, ITERS, iteration, t_ref[pl.ds(local + b, 1), :])
    for q in near_rows:
        wa[q], wv[q] = weight_tables(w_ref, q)


SPLIT = 3
WIDE = 256


def tail_kernel(
    p_ref, w_ref, c_ref, t_ref, own_z, own_x, z1, z2, z3, x1, x2, x3, t_out, panel_out,
    mine, got, out2, got2, t_new, wa, wv, pd, pb, xs, a1, a2,
    s1, r1, s2, r2, s3, r3, ls,
):
    row, col = lax.axis_index("row"), lax.axis_index("col")
    z, x = lax.div(row, 4), lax.rem(row, 4)
    barrier = pltpu.get_barrier_semaphore()
    for j in range(1, ROWS):
        pl.semaphore_signal(barrier, inc=1, device_id={"row": lax.rem(row + j, ROWS)}, device_id_type=MESH)
    local = [pltpu.make_async_copy(own_z, mine.at[0], ls.at[0]), pltpu.make_async_copy(own_x, mine.at[1], ls.at[1])]
    for c in local:
        c.start()
    pl.semaphore_wait(barrier, ROWS - 1)

    def peer(j, along_z):
        return lax.rem(z + j, 4) * 4 + x if along_z else z * 4 + lax.rem(x + j, 4)

    def exchange(sources, target, send, recv, swap):
        copies = []
        for i, source in enumerate(sources):
            copies.append(
                pltpu.make_async_remote_copy(
                    src_ref=source,
                    dst_ref=target.at[i],
                    send_sem=send.at[i],
                    recv_sem=recv.at[i],
                    device_id={"row": peer(i % 3 + 1, (i < 3) != swap)},
                    device_id_type=MESH,
                )
            )
        for i in (1, 4, 0, 3, 2, 5):
            copies[i].start()
        return copies

    first_copies = exchange((z1, z2, z3, x1, x2, x3), got, s1, r1, False)

    def fill(q, _):
        wa[q], wv[q] = weight_tables(w_ref, q)
        return 0

    lax.fori_loop(0, PAIRS, fill, 0, unroll=4)
    first = col * 64 + row * 4

    def block(b, _):
        root_block(b, first, row * 4, p_ref, w_ref, c_ref, t_ref, t_new, wa, wv, pd, pb, xs, a1, a2)
        return 0

    lax.fori_loop(0, SPLIT, block, 0)
    for c in local:
        c.wait()
    for c in first_copies:
        c.wait()

    def add(i, _):
        lanes = pl.ds(pl.multiple_of(i * WIDE, WIDE), WIDE)
        for half in range(2):
            me = x if half == 0 else z
            for j in range(4):
                at = pl.ds(pl.multiple_of(lax.rem(me + j, 4) * 48, 48), 48)
                total = mine[half, at, lanes]
                for k in range(3):
                    total = total + got[half * 3 + k, at, lanes].astype(F32)
                if j:
                    out2[half * 3 + j - 1, :, lanes] = total
                else:
                    panel_out[half, :, lanes] = total
        return 0

    lax.fori_loop(0, PANEL // WIDE, add, 0)
    second_copies = exchange([out2.at[i] for i in range(6)], got2, s2, r2, True)
    lax.fori_loop(SPLIT, 4, block, 0)
    own = pltpu.make_async_copy(t_new, t_out.at[row], ls.at[2])
    own.start()
    third = spread(t_new, t_out, "row", ROWS, row, s3, r3)
    for c in second_copies:
        c.wait()

    def last_add(i, _):
        lanes = pl.ds(pl.multiple_of(i * WIDE, WIDE), WIDE)
        for half in range(2):
            total = panel_out[half, :, lanes]
            for k in range(3):
                total = total + got2[half * 3 + k, :, lanes]
            panel_out[half, :, lanes] = total
        return 0

    lax.fori_loop(0, PANEL // WIDE, last_add, 0)
    collect(third, t_new, t_out, "row", ROWS, row, s3, r3)
    own.wait()


def tail(poles, weights, centers, offsets, blocks):
    anywhere = pl.BlockSpec(memory_space=pl.ANY)
    return pl.pallas_call(
        tail_kernel,
        name="tail",
        out_shape=(jax.ShapeDtypeStruct((ROWS, 4, 128), F32), jax.ShapeDtypeStruct((2, 48, PANEL), F32)),
        in_specs=[vmem()] * 4 + [anywhere] * 8,
        out_specs=(vmem(), vmem()),
        scratch_shapes=[
            VMEM((2, 192, PANEL), F32),
            VMEM((6, 192, PANEL), BF16),
            VMEM((6, 48, PANEL), F32),
            VMEM((6, 48, PANEL), F32),
            VMEM((4, 128), F32),
            VMEM((PAIRS, 8, 256), BF16),
            VMEM((PAIRS, 8, 256), BF16),
            VMEM((TILES, 128), F32),
            VMEM((PAIRS, 8, 256), BF16),
            VMEM((128, 128), F32),
            VMEM((128, 128), F32),
            VMEM((128, 128), F32),
            dma(6), dma(6), dma(6), dma(6), dma(15), dma(15), dma(3),
        ],
        compiler_params=pltpu.CompilerParams(collective_id=2, has_side_effects=True),
    )(poles, weights, centers, offsets, *blocks)


def on_device(pole_values, weights, centers, offsets, chosen, column_pole, eigen_blocks):
    all_p, all_w, all_o = gather_all(pole_values, weights, offsets)
    all_p, all_w, all_o = (a.reshape(TILES, 128) for a in (all_p, all_w, all_o))
    tbl, pw = share(*panel_roots(chosen, all_p, all_w, all_o, column_pole))
    halves = jnp.transpose(eigen_blocks, (1, 0, 2))
    blocks = product(tbl.reshape(128, 128), pw, halves)
    blocks = (blocks[0], blocks[4], *blocks[1:4], *blocks[5:8])
    t, panel = tail(all_p, all_w, centers.reshape(64, 128), offsets.reshape(64, 128), blocks)
    return t.reshape(8192), jnp.transpose(panel, (1, 0, 2))


def solution(mesh):
    placed = (P("row"), P("row"), P("col"), P("col"), P(), P(None, "row"), P("col", None, "row"))
    return jax.shard_map(
        on_device,
        mesh=mesh,
        in_specs=placed,
        out_specs=(P("col"), P(("col", "row"), None, None)),
        check_vma=False,
    )
```
